32 devices in a mesh: rows: 8 (over z, x), ka: 4 (over y, core).
Axes of the slice: x: 2, y: 2, z: 4, core: 2. Of those that a mesh axis runs over, the one named last changes fastest.
Arguments:
- pair_repr: bfloat16 [512, 512, 128], P('rows', 'ka'), may hold values from -6 to 6
- pair_mask: int32 [512, 512], P('rows', 'ka'), may hold values 0 or 1
- ln_gain: float32 [128], replicated, may hold values from 0.1 to 1.9
- ln_bias: float32 [128], replicated, may hold values from -3 to 3
- w_proj: bfloat16 [128, 256], replicated, may hold values from -0.5 to 0.5
- w_gate: bfloat16 [128, 256], replicated, may hold values from -0.5 to 0.5
- w_out_gate: bfloat16 [128, 128], replicated, may hold values from -0.5 to 0.5
- out_gain: float32 [128], replicated, may hold values from 0.1 to 1.9
- out_bias: float32 [128], replicated, may hold values from -3 to 3
- w_out: bfloat16 [128, 128], replicated, may hold values from -0.5 to 0.5
Outputs:
- update: bfloat16 [512, 512, 128], P('rows', 'ka')
The draws below stay inside these ranges and needn't reach their ends.
All inputs are finite; a program needn't handle non-finite values. No bound on the sum of `pair_mask` on one device may be relied on, other than what follows from the above.
Results may differ from the reference program's by a relative error of at most 0.015.
Values may be sent and summed in bfloat16 or wider, within the bound.
A program may use at most 64 MiB of HBM per device.

```python
import jax
import jax.numpy as jnp
from jax import lax

C = 128
H = 128
N = 512


def place_ends(drawn, own_key, smallest, high):
    spot = [jax.random.randint(jax.random.fold_in(own_key, axis), (), 0, length) for axis, length in enumerate(drawn.shape)]
    widest = drawn.shape.index(max(drawn.shape))
    beside = spot[:widest] + [(spot[widest] + 1) % drawn.shape[widest]] + spot[widest + 1:]
    return drawn.at[tuple(spot)].set(smallest).at[tuple(beside)].set(high)


def shard_levels(own_key, extent, shards, least, high):
    def one(position, parts):
        steps = jax.random.uniform(jax.random.fold_in(jax.random.fold_in(own_key, 6), position), (parts,), jnp.float32, least / len(shards), high / len(shards))
        return jnp.repeat(jnp.exp(steps), extent[position] // parts).reshape((-1,) + (1,) * (len(extent) - position - 1))

    loudness = one(*shards[0])
    for cut in shards[1:]:
        loudness = loudness * one(*cut)
    return loudness


def bell_draw(key, dims, deviation, reach, shards=(), held_as=jnp.bfloat16):
    array = jax.random.normal(key, dims, jnp.float32) * deviation
    if len(shards) > 0:
        array = shard_levels(key, dims, shards, -0.22, 0.18) * array
    return jnp.clip(array, min=-reach, max=reach).astype(held_as)


def setup_inputs(seed: int = 0) -> dict:
    seeds = jax.random.split(jax.random.key(seed), 11)
    pair_repr = bell_draw(seeds[0], (N, N, C), 1.0, 6.0, ((0, 8), (1, 4)))
    pair_mask = place_ends((jax.random.randint(seeds[1], (N, N), 0, 4) < 3).astype(jnp.int32), jax.random.fold_in(seeds[1], 1), 0, 1)
    ln_gain = jnp.clip(1.0 + 0.18 * jax.random.normal(seeds[2], (C,), jnp.float32), 0.1, 1.9)
    ln_bias = bell_draw(seeds[3], (C,), 0.5, 3.0, (), jnp.float32)
    w_proj = bell_draw(seeds[4], (C, 2 * H), C ** -0.5, 0.5)
    w_gate = bell_draw(seeds[5], (C, 2 * H), C ** -0.5, 0.5)
    w_out_gate = bell_draw(seeds[6], (C, C), C ** -0.5, 0.5)
    out_gain = jnp.clip(1.0 + 0.18 * jax.random.normal(seeds[7], (H,), jnp.float32), 0.1, 1.9)
    out_bias = bell_draw(seeds[8], (H,), 0.5, 3.0, (), jnp.float32)
    w_out = bell_draw(seeds[9], (H, C), H ** -0.5, 0.5)
    return dict(pair_repr=pair_repr, pair_mask=pair_mask, ln_gain=ln_gain, ln_bias=ln_bias, w_proj=w_proj, w_gate=w_gate, w_out_gate=w_out_gate, out_gain=out_gain, out_bias=out_bias, w_out=w_out)


def layer_norm(values, gain_vec, bias_vec):
    center = lax.optimization_barrier(jnp.mean(values, axis=-1, keepdims=True))
    deviate = values - center
    spread = lax.optimization_barrier(jnp.mean(deviate * deviate, axis=-1, keepdims=True))
    return deviate * lax.rsqrt(spread + 1e-05) * gain_vec + bias_vec

def reference(pair_repr, pair_mask, ln_gain, ln_bias, w_proj, w_gate, w_out_gate, out_gain, out_bias, w_out):
    normed = layer_norm(pair_repr.astype(jnp.float32), ln_gain, ln_bias).astype(jnp.bfloat16)
    flat_rows = normed.reshape(N * N, C)
    projected = jnp.dot(flat_rows, w_proj, preferred_element_type=jnp.float32)
    gate_logits = jnp.dot(flat_rows, w_gate, preferred_element_type=jnp.float32)
    mask_col = pair_mask.reshape(N * N, 1).astype(jnp.float32)
    edges = (jax.nn.sigmoid(gate_logits) * projected * mask_col).astype(jnp.bfloat16).reshape(N, N, 2 * H)
    left_edge = jnp.transpose(edges[:, :, :H], (2, 0, 1)).astype(jnp.float32)
    right_edge = jnp.transpose(edges[:, :, H:], (2, 1, 0)).astype(jnp.float32)
    triangle = jnp.transpose(jnp.matmul(left_edge, right_edge), (1, 2, 0))
    tri_normed = layer_norm(triangle, out_gain, out_bias).astype(jnp.bfloat16)
    out_gate = jax.nn.sigmoid(jnp.dot(flat_rows, w_out_gate, preferred_element_type=jnp.float32))
    projected_out = jnp.dot(tri_normed.reshape(N * N, H), w_out, preferred_element_type=jnp.float32)
    return (out_gate * projected_out).astype(jnp.bfloat16).reshape(N, N, C)
```

```python
import functools

import jax
import jax.numpy as jnp
from jax import lax
from jax.experimental import pallas as pl
from jax.experimental.pallas import tpu as pltpu
from jax.sharding import PartitionSpec as P

MESH = pl.DeviceIdType.MESH
CHUNK = 16


def layer_norm(values, gain_vec, bias_vec):
    center = jnp.mean(values, axis=-1, keepdims=True)
    deviate = values - center
    spread = jnp.mean(deviate * deviate, axis=-1, keepdims=True)
    return deviate * lax.rsqrt(spread + 1e-05) * gain_vec + bias_vec


def sigmoid(logits):
    return 0.5 + 0.5 * jnp.tanh(0.5 * logits)


def kernel(
    rows_n, ka_n, halves,
    pair_ref, mask_ref, ln_gain_ref, ln_bias_ref, w_proj_ref, w_gate_ref, w_out_gate_ref,
    out_gain_ref, out_bias_ref, w_out_ref,
    out_ref,
    edges, wide, normed, gates, left, right, tri, back, w_cat, gain_col, bias_col,
    recv_lr, send_left, send_right, recv_tri, send_tri,
):
    row = lax.axis_index("rows")
    col = lax.axis_index("ka")
    row_count, col_count, chans = pair_ref.shape
    hidden = w_out_ref.shape[0]
    group_rows = rows_n // halves
    members = group_rows * ka_n
    share = hidden // members
    half = row // group_rows
    spot = row % group_rows
    member = spot * ka_n + col
    chunks = row_count // CHUNK

    barrier = pltpu.get_barrier_semaphore()

    def greet(step, carry):
        to_row = (row + step // ka_n) % rows_n
        to_col = (col + step % ka_n) % ka_n
        pl.semaphore_signal(barrier, inc=1, device_id=(to_row, to_col), device_id_type=MESH)
        return carry

    lax.fori_loop(1, rows_n * ka_n, greet, 0)

    def turned(ref):
        return ref[...].astype(jnp.float32).T.astype(jnp.bfloat16)

    w_cat[: 2 * hidden, :] = turned(w_gate_ref)
    w_cat[2 * hidden :, :] = turned(w_proj_ref)
    gain_col[...] = jnp.broadcast_to(out_gain_ref[...], (col_count, hidden)).T
    bias_col[...] = jnp.broadcast_to(out_bias_ref[...], (col_count, hidden)).T

    def left_copy(chunk, to_spot, to_col):
        to_member = to_spot * ka_n + to_col
        return pltpu.make_async_remote_copy(
            src_ref=edges.at[pl.ds(to_member * share, share), pl.ds(chunk * CHUNK, CHUNK), :],
            dst_ref=left.at[
                :, pl.ds(spot * row_count + chunk * CHUNK, CHUNK), pl.ds(pl.multiple_of(col * col_count, 128), col_count)
            ],
            send_sem=send_left,
            recv_sem=recv_lr.at[0],
            device_id=(half * group_rows + to_spot, to_col),
            device_id_type=MESH,
        )

    def right_copy(chunk, turn, to_spot, to_col):
        to_member = to_spot * ka_n + to_col
        to_half = (half + turn) % halves
        return pltpu.make_async_remote_copy(
            src_ref=edges.at[
                pl.ds(hidden + to_member * share, share), pl.ds(chunk * CHUNK, CHUNK), :
            ],
            dst_ref=right.at[
                :, pl.ds(row * row_count + chunk * CHUNK, CHUNK), pl.ds(pl.multiple_of(col * col_count, 128), col_count)
            ],
            send_sem=send_right.at[turn],
            recv_sem=recv_lr.at[1],
            device_id=(to_half * group_rows + to_spot, to_col),
            device_id_type=MESH,
        )

    def partner(step):
        return (spot + step // ka_n) % group_rows, (col + step % ka_n) % ka_n

    def make_chunk(chunk):
        def one_row(local, carry):
            at = chunk * CHUNK + local
            values = pair_ref[at].astype(jnp.float32)
            plain = layer_norm(values, ln_gain_ref[...], ln_bias_ref[...]).astype(jnp.bfloat16)
            normed[at] = plain
            both = lax.dot_general(
                w_cat[...], plain, (((1,), (1,)), ((), ())), preferred_element_type=jnp.float32
            )
            mask_row = mask_ref[pl.ds(at, 1), :].astype(jnp.float32)
            made = sigmoid(both[: 2 * hidden]) * both[2 * hidden :] * mask_row
            wide[pl.ds(local, 2 * hidden, stride=CHUNK), :] = made
            return carry

        lax.fori_loop(0, CHUNK, one_row, 0, unroll=2)
        packed = wide[...].reshape(2 * hidden, CHUNK, col_count).astype(jnp.bfloat16)
        edges[:, pl.ds(pl.multiple_of(chunk * CHUNK, CHUNK), CHUNK), :] = packed

    def send_chunk(chunk):
        def far(step, carry):
            for turn in range(1, halves):
                right_copy(chunk, turn, *partner(step)).start()
            return carry

        lax.fori_loop(0, members, far, 0)

        def near(step, carry):
            to_spot, to_col = partner(step)
            left_copy(chunk, to_spot, to_col).start()
            right_copy(chunk, 0, to_spot, to_col).start()
            return carry

        lax.fori_loop(1, members, near, 0)

    make_chunk(0)
    pl.semaphore_wait(barrier, rows_n * ka_n - 1)
    send_chunk(0)

    def rest(chunk, carry):
        make_chunk(chunk)
        send_chunk(chunk)
        return carry

    lax.fori_loop(1, chunks, rest, 0)

    own_cols = pl.ds(pl.multiple_of(col * col_count, 128), col_count)
    pltpu.make_async_copy(
        edges.at[pl.ds(member * share, share)],
        left.at[:, pl.ds(spot * row_count, row_count), own_cols],
        recv_lr.at[0],
    ).start()
    pltpu.make_async_copy(
        edges.at[pl.ds(hidden + member * share, share)],
        right.at[:, pl.ds(row * row_count, row_count), own_cols],
        recv_lr.at[1],
    ).start()

    def gate_row(at, carry):
        gates[at] = sigmoid(
            jnp.dot(normed[at], w_out_gate_ref[...], preferred_element_type=jnp.float32)
        )
        return carry

    lax.fori_loop(0, row_count, gate_row, 0, unroll=2)

    pltpu.make_async_copy(left, left, recv_lr.at[0]).wait()
    pltpu.make_async_copy(right, right, recv_lr.at[1]).wait()

    def tri_src(chan, to_spot, to_col):
        return tri.at[
            chan, pl.ds(to_spot * row_count, row_count), pl.ds(pl.multiple_of(to_col * col_count, 128), col_count)
        ]

    def one_channel(chan, carry):
        tri[chan] = lax.dot_general(
            left[chan], right[chan], (((1,), (1,)), ((), ())), preferred_element_type=jnp.float32
        ).astype(jnp.bfloat16)
        slot = back.at[member * share + chan]

        def give(step, inner):
            to_spot, to_col = partner(step)
            pltpu.make_async_remote_copy(
                src_ref=tri_src(chan, to_spot, to_col),
                dst_ref=slot,
                send_sem=send_tri,
                recv_sem=recv_tri,
                device_id=(half * group_rows + to_spot, to_col),
                device_id_type=MESH,
            ).start()
            return inner

        lax.fori_loop(1, members, give, 0)
        pltpu.make_async_copy(tri_src(chan, spot, col), slot, recv_tri).start()
        return carry

    lax.fori_loop(0, share, one_channel, 0)

    pltpu.make_async_copy(back, back, recv_tri).wait()

    def finish(chunk, carry):
        first = pl.multiple_of(chunk * CHUNK, CHUNK)
        sums = back[:, pl.ds(first, CHUNK), :].astype(jnp.float32)
        center = jnp.mean(sums, axis=0, keepdims=True)
        deviate = sums - center
        spread = jnp.mean(deviate * deviate, axis=0, keepdims=True)
        scaled = deviate * lax.rsqrt(spread + 1e-05)
        wide[: hidden * CHUNK, :] = scaled.reshape(hidden * CHUNK, col_count)

        def one_row(local, inner):
            at = first + local
            chans_first = wide[pl.ds(local, hidden, stride=CHUNK), :]
            tri_normed = (chans_first * gain_col[...] + bias_col[...]).astype(jnp.bfloat16)
            projected = lax.dot_general(
                tri_normed, w_out_ref[...], (((0,), (0,)), ((), ())), preferred_element_type=jnp.float32
            )
            out_ref[at] = (gates[at] * projected).astype(jnp.bfloat16)
            return inner

        lax.fori_loop(0, CHUNK, one_row, 0, unroll=2)
        return carry

    lax.fori_loop(0, chunks, finish, 0)

    others = pl.ds(0, (members - 1) * share)
    pltpu.make_async_copy(edges.at[others], edges.at[others], send_left).wait()
    pltpu.make_async_copy(edges.at[others], edges.at[others], send_right.at[0]).wait()
    for turn in range(1, halves):
        every = pl.ds(0, hidden)
        pltpu.make_async_copy(edges.at[every], edges.at[every], send_right.at[turn]).wait()
    pltpu.make_async_copy(back.at[others], back.at[others], send_tri).wait()


def fused(rows_n, ka_n, halves, args):
    pair_repr, pair_mask, ln_gain, ln_bias, w_proj, w_gate, w_out_gate, out_gain, out_bias, w_out = args
    row_count, col_count, chans = pair_repr.shape
    hidden = w_out.shape[0]
    members = rows_n // halves * ka_n
    share = hidden // members
    half = jnp.bfloat16
    return pl.pallas_call(
        functools.partial(kernel, rows_n, ka_n, halves),
        out_shape=jax.ShapeDtypeStruct(pair_repr.shape, half),
        in_specs=[pl.BlockSpec(memory_space=pltpu.VMEM)] * 10,
        out_specs=pl.BlockSpec(memory_space=pltpu.VMEM),
        scratch_shapes=[
            pltpu.VMEM((2 * hidden, row_count, col_count), half),
            pltpu.VMEM((2 * hidden * CHUNK, col_count), jnp.float32),
            pltpu.VMEM((row_count, col_count, chans), half),
            pltpu.VMEM((row_count, col_count, chans), jnp.float32),
            pltpu.VMEM((share, rows_n // halves * row_count, ka_n * col_count), half),
            pltpu.VMEM((share, rows_n * row_count, ka_n * col_count), half),
            pltpu.VMEM((share, rows_n // halves * row_count, ka_n * col_count), half),
            pltpu.VMEM((hidden, row_count, col_count), half),
            pltpu.VMEM((4 * hidden, chans), half),
            pltpu.VMEM((hidden, col_count), jnp.float32),
            pltpu.VMEM((hidden, col_count), jnp.float32),
            pltpu.SemaphoreType.DMA((2,)),
            pltpu.SemaphoreType.DMA,
            pltpu.SemaphoreType.DMA((halves,)),
            pltpu.SemaphoreType.DMA,
            pltpu.SemaphoreType.DMA,
        ],
        compiler_params=pltpu.CompilerParams(
            collective_id=0, has_side_effects=True, vmem_limit_bytes=60 * 2**20
        ),
    )(
        pair_repr, pair_mask, ln_gain[None], ln_bias[None], w_proj, w_gate, w_out_gate,
        out_gain[None], out_bias[None], w_out,
    )


def plain(args):
    pair_repr, pair_mask, ln_gain, ln_bias, w_proj, w_gate, w_out_gate, out_gain, out_bias, w_out = args
    row_count, col_count, chans = pair_repr.shape
    hidden = w_out.shape[0]
    normed = layer_norm(pair_repr.astype(jnp.float32), ln_gain, ln_bias).astype(jnp.bfloat16)
    flat_rows = normed.reshape(row_count * col_count, chans)
    projected = jnp.dot(flat_rows, w_proj, preferred_element_type=jnp.float32)
    gate_logits = jnp.dot(flat_rows, w_gate, preferred_element_type=jnp.float32)
    mask_col = pair_mask.reshape(row_count * col_count, 1).astype(jnp.float32)
    edges = (jax.nn.sigmoid(gate_logits) * projected * mask_col).astype(jnp.bfloat16)
    edges = edges.reshape(row_count, col_count, 2 * hidden)
    partial_sums = jnp.einsum(
        "ikh,jkh->ijh",
        edges[:, :, :hidden],
        lax.all_gather(edges[:, :, hidden:], "rows", axis=0, tiled=True),
        preferred_element_type=jnp.float32,
    )
    triangle = lax.psum_scatter(
        partial_sums.astype(jnp.bfloat16), "ka", scatter_dimension=1, tiled=True
    ).astype(jnp.float32)
    tri_normed = layer_norm(triangle, out_gain, out_bias).astype(jnp.bfloat16)
    out_gate = jax.nn.sigmoid(jnp.dot(flat_rows, w_out_gate, preferred_element_type=jnp.float32))
    projected_out = jnp.dot(
        tri_normed.reshape(row_count * col_count, hidden), w_out, preferred_element_type=jnp.float32
    )
    return (out_gate * projected_out).astype(jnp.bfloat16).reshape(row_count, col_count, chans)


def body(rows_n, ka_n, *args):
    row_count, col_count, chans = args[0].shape
    hidden = args[-1].shape[0]
    halves = 2 if rows_n % 2 == 0 else 1
    members = rows_n // halves * ka_n
    aligned = row_count % CHUNK == 0 and col_count % 128 == 0 and chans % 128 == 0 and hidden % 128 == 0
    if aligned and hidden % members == 0 and col_count == hidden:
        return fused(rows_n, ka_n, halves, args)
    return plain(args)


def solution(mesh):
    placed = (P("rows", "ka", None), P("rows", "ka"), P(), P(), P(), P(), P(), P(), P(), P())
    return jax.shard_map(
        functools.partial(body, mesh.shape["rows"], mesh.shape["ka"]),
        mesh=mesh, in_specs=placed, out_specs=P("rows", "ka", None), check_vma=False,
    )
```

```python
import functools

import jax
import jax.numpy as jnp
from jax import lax
from jax.experimental import pallas as pl
from jax.experimental.pallas import tpu as pltpu
from jax.sharding import PartitionSpec as P

MESH = pl.DeviceIdType.MESH
CHUNK = 16
PITCH = 24


def layer_norm(values, gain_vec, bias_vec):
    center = jnp.mean(values, axis=-1, keepdims=True)
    deviate = values - center
    spread = jnp.mean(deviate * deviate, axis=-1, keepdims=True)
    return deviate * lax.rsqrt(spread + 1e-05) * gain_vec + bias_vec


def sigmoid(logits):
    return 0.5 + 0.5 * jnp.tanh(0.5 * logits)


def kernel(
    rows_n, ka_n, halves, groups,
    pair_hbm, mask_ref, ln_gain_ref, ln_bias_ref, w_proj_ref, w_gate_ref, w_out_gate_ref,
    out_gain_ref, out_bias_ref, w_out_ref,
    out_hbm,
    pair_ref, out_ref, edges, wide, normed, gates, left, right, tri, back, w_cat, gain_col, bias_col,
    load_sem, store_sem, recv_left, recv_right, send_left, send_right, recv_tri, send_tri,
):
    row = lax.axis_index("rows")
    col = lax.axis_index("ka")
    row_count, col_count, chans = pair_ref.shape
    hidden = w_out_ref.shape[0]
    group_rows = rows_n // halves
    members = group_rows * ka_n
    share = hidden // members
    half = row // group_rows
    spot = row % group_rows
    member = spot * ka_n + col
    chunks = row_count // CHUNK

    sub = share // groups
    planes = wide.reshape(2 * hidden, PITCH, col_count)

    def chunk_rows(chunk):
        return pl.ds(pl.multiple_of(chunk * CHUNK, CHUNK), CHUNK)

    def load(chunk):
        rows = chunk_rows(chunk)
        return pltpu.make_async_copy(pair_hbm.at[rows], pair_ref.at[rows], load_sem.at[chunk])

    for chunk in range(chunks):
        load(chunk).start()

    barrier = pltpu.get_barrier_semaphore()

    def greet(step, carry):
        to_row = (row + step // ka_n) % rows_n
        to_col = (col + step % ka_n) % ka_n
        pl.semaphore_signal(barrier, inc=1, device_id=(to_row, to_col), device_id_type=MESH)
        return carry

    lax.fori_loop(1, rows_n * ka_n, greet, 0)

    def turned(ref):
        return ref[...].astype(jnp.float32).T.astype(jnp.bfloat16)

    w_cat[: 2 * hidden, :] = turned(w_gate_ref)
    w_cat[2 * hidden :, :] = turned(w_proj_ref)

    own_cols = pl.ds(pl.multiple_of(col * col_count, 128), col_count)

    def left_copy(group, first, size, to_spot, to_col):
        to_member = to_spot * ka_n + to_col
        return pltpu.make_async_remote_copy(
            src_ref=edges.at[pl.ds(to_member * share + group * sub, sub), pl.ds(first, size), :],
            dst_ref=left.at[pl.ds(group * sub, sub), pl.ds(spot * row_count + first, size), own_cols],
            send_sem=send_left,
            recv_sem=recv_left.at[group],
            device_id=(half * group_rows + to_spot, to_col),
            device_id_type=MESH,
        )

    def right_copy(group, first, size, turn, to_spot, to_col):
        to_member = to_spot * ka_n + to_col
        to_half = (half + turn) % halves
        return pltpu.make_async_remote_copy(
            src_ref=edges.at[
                pl.ds(hidden + to_member * share + group * sub, sub), pl.ds(first, size), :
            ],
            dst_ref=right.at[pl.ds(group * sub, sub), pl.ds(row * row_count + first, size), own_cols],
            send_sem=send_right.at[turn],
            recv_sem=recv_right.at[group],
            device_id=(to_half * group_rows + to_spot, to_col),
            device_id_type=MESH,
        )

    def partner(step):
        return (spot + step // ka_n) % group_rows, (col + step % ka_n) % ka_n

    def make_chunk(chunk):
        load(chunk).wait()

        def one_row(local, carry):
            at = chunk * CHUNK + local
            values = pair_ref[at].astype(jnp.float32)
            plain = layer_norm(values, ln_gain_ref[...], ln_bias_ref[...]).astype(jnp.bfloat16)
            normed[at] = plain
            both = lax.dot_general(
                w_cat[...], plain, (((1,), (1,)), ((), ())), preferred_element_type=jnp.float32
            )
            mask_row = mask_ref[pl.ds(at, 1), :].astype(jnp.float32)
            made = sigmoid(both[: 2 * hidden]) * both[2 * hidden :] * mask_row
            wide[pl.ds(local, 2 * hidden, stride=PITCH), :] = made
            return carry

        lax.fori_loop(0, CHUNK, one_row, 0, unroll=2)
        edges[:, chunk_rows(chunk), :] = planes[:, :CHUNK, :].astype(jnp.bfloat16)

    def send_part(group, first, size):
        def far(step, carry):
            for turn in range(1, halves):
                right_copy(group, first, size, turn, *partner(step)).start()
            return carry

        lax.fori_loop(0, members, far, 0)

        def near(step, carry):
            to_spot, to_col = partner(step)
            left_copy(group, first, size, to_spot, to_col).start()
            right_copy(group, first, size, 0, to_spot, to_col).start()
            return carry

        lax.fori_loop(1, members, near, 0)

    def send_chunk(chunk):
        send_part(0, pl.multiple_of(chunk * CHUNK, CHUNK), CHUNK)

    make_chunk(0)
    pl.semaphore_wait(barrier, rows_n * ka_n - 1)
    send_chunk(0)

    def rest(chunk, carry):
        make_chunk(chunk)
        send_chunk(chunk)
        return carry

    lax.fori_loop(1, chunks, rest, 0)

    for group in range(1, groups):
        send_part(group, 0, row_count)

    for group in range(groups):
        mine = pl.ds(group * sub, sub)
        pltpu.make_async_copy(
            edges.at[pl.ds(member * share + group * sub, sub)],
            left.at[mine, pl.ds(spot * row_count, row_count), own_cols],
            recv_left.at[group],
        ).start()
        pltpu.make_async_copy(
            edges.at[pl.ds(hidden + member * share + group * sub, sub)],
            right.at[mine, pl.ds(row * row_count, row_count), own_cols],
            recv_right.at[group],
        ).start()

    gain_col[...] = jnp.broadcast_to(out_gain_ref[...], (col_count, hidden)).T
    bias_col[...] = jnp.broadcast_to(out_bias_ref[...], (col_count, hidden)).T

    def gate_row(at, carry):
        gates[at] = sigmoid(
            jnp.dot(normed[at], w_out_gate_ref[...], preferred_element_type=jnp.float32)
        )
        return carry

    lax.fori_loop(0, row_count, gate_row, 0, unroll=2)

    def one_channel(chan, carry):
        tri[chan] = lax.dot_general(
            left[chan], right[chan], (((1,), (1,)), ((), ())), preferred_element_type=jnp.float32
        ).astype(jnp.bfloat16)
        return carry

    def tri_part(group, chunk, to_spot, to_col):
        return tri.at[
            pl.ds(group * sub, sub),
            pl.ds(to_spot * row_count + chunk * CHUNK, CHUNK),
            pl.ds(pl.multiple_of(to_col * col_count, 128), col_count),
        ]

    for group in range(groups):
        mine = pl.ds(group * sub, sub)
        pltpu.make_async_copy(left.at[mine], left.at[mine], recv_left.at[group]).wait()
        pltpu.make_async_copy(right.at[mine], right.at[mine], recv_right.at[group]).wait()
        lax.fori_loop(group * sub, (group + 1) * sub, one_channel, 0)

        def give_chunk(chunk, carry):
            slot = back.at[pl.ds(member * share + group * sub, sub), chunk_rows(chunk), :]

            def give(step, inner):
                to_spot, to_col = partner(step)
                pltpu.make_async_remote_copy(
                    src_ref=tri_part(group, chunk, to_spot, to_col),
                    dst_ref=slot,
                    send_sem=send_tri,
                    recv_sem=recv_tri.at[chunk],
                    device_id=(half * group_rows + to_spot, to_col),
                    device_id_type=MESH,
                ).start()
                return inner

            lax.fori_loop(1, members, give, 0)
            pltpu.make_async_copy(
                tri_part(group, chunk, spot, col), slot, recv_tri.at[chunk]
            ).start()
            return carry

        lax.fori_loop(0, chunks, give_chunk, 0)

    def finish(chunk, carry):
        first = pl.multiple_of(chunk * CHUNK, CHUNK)
        arrived = back.at[:, chunk_rows(chunk), :]
        pltpu.make_async_copy(arrived, arrived, recv_tri.at[chunk]).wait()
        sums = back[:, pl.ds(first, CHUNK), :].astype(jnp.float32)
        center = jnp.mean(sums, axis=0, keepdims=True)
        deviate = sums - center
        spread = jnp.mean(deviate * deviate, axis=0, keepdims=True)
        scaled = deviate * lax.rsqrt(spread + 1e-05)
        planes[:hidden, :CHUNK, :] = scaled

        def one_row(local, inner):
            at = first + local
            chans_first = wide[pl.ds(local, hidden, stride=PITCH), :]
            tri_normed = (chans_first * gain_col[...] + bias_col[...]).astype(jnp.bfloat16)
            projected = lax.dot_general(
                tri_normed, w_out_ref[...], (((0,), (0,)), ((), ())), preferred_element_type=jnp.float32
            )
            out_ref[at] = (gates[at] * projected).astype(jnp.bfloat16)
            return inner

        lax.fori_loop(0, CHUNK, one_row, 0, unroll=2)
        pltpu.make_async_copy(
            out_ref.at[chunk_rows(chunk)], out_hbm.at[chunk_rows(chunk)], store_sem
        ).start()
        return carry

    lax.fori_loop(0, chunks, finish, 0)
    pltpu.make_async_copy(out_ref, out_hbm, store_sem).wait()

    others = pl.ds(0, (members - 1) * share)
    pltpu.make_async_copy(edges.at[others], edges.at[others], send_left).wait()
    pltpu.make_async_copy(edges.at[others], edges.at[others], send_right.at[0]).wait()
    for turn in range(1, halves):
        every = pl.ds(0, hidden)
        pltpu.make_async_copy(edges.at[every], edges.at[every], send_right.at[turn]).wait()
    pltpu.make_async_copy(back.at[others], back.at[others], send_tri).wait()


def fused(rows_n, ka_n, halves, args):
    pair_repr, pair_mask, ln_gain, ln_bias, w_proj, w_gate, w_out_gate, out_gain, out_bias, w_out = args
    row_count, col_count, chans = pair_repr.shape
    hidden = w_out.shape[0]
    members = rows_n // halves * ka_n
    share = hidden // members
    groups = 2 if share % 2 == 0 else 1
    half = jnp.bfloat16
    return pl.pallas_call(
        functools.partial(kernel, rows_n, ka_n, halves, groups),
        out_shape=jax.ShapeDtypeStruct(pair_repr.shape, half),
        in_specs=[pl.BlockSpec(memory_space=pl.ANY)] + [pl.BlockSpec(memory_space=pltpu.VMEM)] * 9,
        out_specs=pl.BlockSpec(memory_space=pl.ANY),
        scratch_shapes=[
            pltpu.VMEM((row_count, col_count, chans), half),
            pltpu.VMEM((row_count, col_count, chans), half),
            pltpu.VMEM((2 * hidden, row_count, col_count), half),
            pltpu.VMEM((2 * hidden * PITCH, col_count), jnp.float32),
            pltpu.VMEM((row_count, col_count, chans), half),
            pltpu.VMEM((row_count, col_count, chans), jnp.float32),
            pltpu.VMEM((share, rows_n // halves * row_count, ka_n * col_count), half),
            pltpu.VMEM((share, rows_n * row_count, ka_n * col_count), half),
            pltpu.VMEM((share, rows_n // halves * row_count, ka_n * col_count), half),
            pltpu.VMEM((hidden, row_count, col_count), half),
            pltpu.VMEM((4 * hidden, chans), half),
            pltpu.VMEM((hidden, col_count), jnp.float32),
            pltpu.VMEM((hidden, col_count), jnp.float32),
            pltpu.SemaphoreType.DMA((row_count // CHUNK,)),
            pltpu.SemaphoreType.DMA,
            pltpu.SemaphoreType.DMA((groups,)),
            pltpu.SemaphoreType.DMA((groups,)),
            pltpu.SemaphoreType.DMA,
            pltpu.SemaphoreType.DMA((halves,)),
            pltpu.SemaphoreType.DMA((row_count // CHUNK,)),
            pltpu.SemaphoreType.DMA,
        ],
        compiler_params=pltpu.CompilerParams(
            collective_id=0, has_side_effects=True, vmem_limit_bytes=60 * 2**20
        ),
    )(
        pair_repr, pair_mask, ln_gain[None], ln_bias[None], w_proj, w_gate, w_out_gate,
        out_gain[None], out_bias[None], w_out,
    )


def plain(args):
    pair_repr, pair_mask, ln_gain, ln_bias, w_proj, w_gate, w_out_gate, out_gain, out_bias, w_out = args
    row_count, col_count, chans = pair_repr.shape
    hidden = w_out.shape[0]
    normed = layer_norm(pair_repr.astype(jnp.float32), ln_gain, ln_bias).astype(jnp.bfloat16)
    flat_rows = normed.reshape(row_count * col_count, chans)
    projected = jnp.dot(flat_rows, w_proj, preferred_element_type=jnp.float32)
    gate_logits = jnp.dot(flat_rows, w_gate, preferred_element_type=jnp.float32)
    mask_col = pair_mask.reshape(row_count * col_count, 1).astype(jnp.float32)
    edges = (jax.nn.sigmoid(gate_logits) * projected * mask_col).astype(jnp.bfloat16)
    edges = edges.reshape(row_count, col_count, 2 * hidden)
    partial_sums = jnp.einsum(
        "ikh,jkh->ijh",
        edges[:, :, :hidden],
        lax.all_gather(edges[:, :, hidden:], "rows", axis=0, tiled=True),
        preferred_element_type=jnp.float32,
    )
    triangle = lax.psum_scatter(
        partial_sums.astype(jnp.bfloat16), "ka", scatter_dimension=1, tiled=True
    ).astype(jnp.float32)
    tri_normed = layer_norm(triangle, out_gain, out_bias).astype(jnp.bfloat16)
    out_gate = jax.nn.sigmoid(jnp.dot(flat_rows, w_out_gate, preferred_element_type=jnp.float32))
    projected_out = jnp.dot(
        tri_normed.reshape(row_count * col_count, hidden), w_out, preferred_element_type=jnp.float32
    )
    return (out_gate * projected_out).astype(jnp.bfloat16).reshape(row_count, col_count, chans)


def body(rows_n, ka_n, *args):
    row_count, col_count, chans = args[0].shape
    hidden = args[-1].shape[0]
    halves = 2 if rows_n % 2 == 0 else 1
    members = rows_n // halves * ka_n
    aligned = row_count % CHUNK == 0 and col_count % 128 == 0 and chans % 128 == 0 and hidden % 128 == 0
    if aligned and hidden % members == 0 and col_count == hidden:
        return fused(rows_n, ka_n, halves, args)
    return plain(args)


def solution(mesh):
    placed = (P("rows", "ka", None), P("rows", "ka"), P(), P(), P(), P(), P(), P(), P(), P())
    return jax.shard_map(
        functools.partial(body, mesh.shape["rows"], mesh.shape["ka"]),
        mesh=mesh, in_specs=placed, out_specs=P("rows", "ka", None), check_vma=False,
    )
```

```python
import functools

import jax
import jax.numpy as jnp
from jax import lax
from jax.experimental import pallas as pl
from jax.experimental.pallas import tpu as pltpu
from jax.sharding import PartitionSpec as P

MESH = pl.DeviceIdType.MESH
CHUNK = 16
PITCH = 24


def layer_norm(values, gain_vec, bias_vec):
    center = jnp.mean(values, axis=-1, keepdims=True)
    deviate = values - center
    spread = jnp.mean(deviate * deviate, axis=-1, keepdims=True)
    return deviate * lax.rsqrt(spread + 1e-05) * gain_vec + bias_vec


def sigmoid(logits):
    return 0.5 + 0.5 * jnp.tanh(0.5 * logits)


def kernel(
    rows_n, ka_n, halves, groups,
    pair_hbm, mask_ref, ln_gain_ref, ln_bias_ref, w_proj_ref, w_gate_ref, w_out_gate_ref,
    out_gain_ref, out_bias_ref, w_out_ref,
    out_hbm,
    pair_ref, out_ref, edges, wide, normed, gates, left, right, tri, back, w_cat, gain_col, bias_col,
    load_sem, store_sem, recv_left, recv_right, send_left, send_right, recv_tri, send_tri,
):
    row = lax.axis_index("rows")
    col = lax.axis_index("ka")
    row_count, col_count, chans = pair_ref.shape
    hidden = w_out_ref.shape[0]
    group_rows = rows_n // halves
    members = group_rows * ka_n
    share = hidden // members
    half = row // group_rows
    spot = row % group_rows
    member = spot * ka_n + col
    chunks = row_count // CHUNK

    sub = share // groups
    planes = wide.reshape(2 * hidden, PITCH, col_count)

    def chunk_rows(chunk):
        return pl.ds(pl.multiple_of(chunk * CHUNK, CHUNK), CHUNK)

    def load(chunk):
        rows = chunk_rows(chunk)
        return pltpu.make_async_copy(pair_hbm.at[rows], pair_ref.at[rows], load_sem.at[chunk])

    for chunk in range(chunks):
        load(chunk).start()

    barrier = pltpu.get_barrier_semaphore()

    def greet(step, carry):
        to_row = (row + step // ka_n) % rows_n
        to_col = (col + step % ka_n) % ka_n
        pl.semaphore_signal(barrier, inc=1, device_id=(to_row, to_col), device_id_type=MESH)
        return carry

    lax.fori_loop(1, rows_n * ka_n, greet, 0)

    def turned(ref):
        return ref[...].astype(jnp.float32).T.astype(jnp.bfloat16)

    w_cat[: 2 * hidden, :] = turned(w_gate_ref)
    w_cat[2 * hidden :, :] = turned(w_proj_ref)

    own_cols = pl.ds(pl.multiple_of(col * col_count, 128), col_count)

    def left_copy(group, first, size, to_spot, to_col):
        to_member = to_spot * ka_n + to_col
        return pltpu.make_async_remote_copy(
            src_ref=edges.at[pl.ds(to_member * share + group * sub, sub), pl.ds(first, size), :],
            dst_ref=left.at[pl.ds(group * sub, sub), pl.ds(spot * row_count + first, size), own_cols],
            send_sem=send_left,
            recv_sem=recv_left.at[group],
            device_id=(half * group_rows + to_spot, to_col),
            device_id_type=MESH,
        )

    def right_copy(group, first, size, turn, to_spot, to_col):
        to_member = to_spot * ka_n + to_col
        to_half = (half + turn) % halves
        return pltpu.make_async_remote_copy(
            src_ref=edges.at[
                pl.ds(hidden + to_member * share + group * sub, sub), pl.ds(first, size), :
            ],
            dst_ref=right.at[pl.ds(group * sub, sub), pl.ds(row * row_count + first, size), own_cols],
            send_sem=send_right.at[turn],
            recv_sem=recv_right.at[group],
            device_id=(to_half * group_rows + to_spot, to_col),
            device_id_type=MESH,
        )

    def partner(step):
        return (spot + step % group_rows) % group_rows, (col + step // group_rows) % ka_n

    def make_chunk(chunk):
        load(chunk).wait()

        def one_row(local, carry):
            at = chunk * CHUNK + local
            values = pair_ref[at].astype(jnp.float32)
            plain = layer_norm(values, ln_gain_ref[...], ln_bias_ref[...]).astype(jnp.bfloat16)
            normed[at] = plain
            both = lax.dot_general(
                w_cat[...], plain, (((1,), (1,)), ((), ())), preferred_element_type=jnp.float32
            )
            mask_row = mask_ref[pl.ds(at, 1), :].astype(jnp.float32)
            made = sigmoid(both[: 2 * hidden]) * both[2 * hidden :] * mask_row
            wide[pl.ds(local, 2 * hidden, stride=PITCH), :] = made
            return carry

        lax.fori_loop(0, CHUNK, one_row, 0, unroll=2)
        edges[:, chunk_rows(chunk), :] = planes[:, :CHUNK, :].astype(jnp.bfloat16)

    def send_part(group, first, size):
        def near(step, carry):
            to_spot, to_col = partner(step)
            left_copy(group, first, size, to_spot, to_col).start()
            right_copy(group, first, size, 0, to_spot, to_col).start()
            return carry

        lax.fori_loop(1, members, near, 0)

        def far(step, carry):
            for turn in range(1, halves):
                right_copy(group, first, size, turn, *partner(step)).start()
            return carry

        lax.fori_loop(0, members, far, 0)

    def send_chunk(chunk):
        send_part(0, pl.multiple_of(chunk * CHUNK, CHUNK), CHUNK)

    make_chunk(0)
    pl.semaphore_wait(barrier, rows_n * ka_n - 1)
    send_chunk(0)

    def rest(chunk, carry):
        make_chunk(chunk)
        send_chunk(chunk)
        return carry

    lax.fori_loop(1, chunks, rest, 0)

    for group in range(1, groups):
        send_part(group, 0, row_count)

    for group in range(groups):
        mine = pl.ds(group * sub, sub)
        pltpu.make_async_copy(
            edges.at[pl.ds(member * share + group * sub, sub)],
            left.at[mine, pl.ds(spot * row_count, row_count), own_cols],
            recv_left.at[group],
        ).start()
        pltpu.make_async_copy(
            edges.at[pl.ds(hidden + member * share + group * sub, sub)],
            right.at[mine, pl.ds(row * row_count, row_count), own_cols],
            recv_right.at[group],
        ).start()

    gain_col[...] = jnp.broadcast_to(out_gain_ref[...], (col_count, hidden)).T
    bias_col[...] = jnp.broadcast_to(out_bias_ref[...], (col_count, hidden)).T

    def gate_row(at, carry):
        gates[at] = sigmoid(
            jnp.dot(normed[at], w_out_gate_ref[...], preferred_element_type=jnp.float32)
        )
        return carry

    lax.fori_loop(0, row_count, gate_row, 0, unroll=2)

    def one_channel(chan, carry):
        tri[chan] = lax.dot_general(
            left[chan], right[chan], (((1,), (1,)), ((), ())), preferred_element_type=jnp.float32
        ).astype(jnp.bfloat16)
        return carry

    def tri_part(group, chunk, to_spot, to_col):
        return tri.at[
            pl.ds(group * sub, sub),
            pl.ds(to_spot * row_count + chunk * CHUNK, CHUNK),
            pl.ds(pl.multiple_of(to_col * col_count, 128), col_count),
        ]

    for group in range(groups):
        mine = pl.ds(group * sub, sub)
        pltpu.make_async_copy(left.at[mine], left.at[mine], recv_left.at[group]).wait()
        pltpu.make_async_copy(right.at[mine], right.at[mine], recv_right.at[group]).wait()
        lax.fori_loop(group * sub, (group + 1) * sub, one_channel, 0)

        def give_chunk(chunk, carry):
            slot = back.at[pl.ds(member * share + group * sub, sub), chunk_rows(chunk), :]

            def give(step, inner):
                to_spot, to_col = partner(step)
                pltpu.make_async_remote_copy(
                    src_ref=tri_part(group, chunk, to_spot, to_col),
                    dst_ref=slot,
                    send_sem=send_tri,
                    recv_sem=recv_tri.at[chunk],
                    device_id=(half * group_rows + to_spot, to_col),
                    device_id_type=MESH,
                ).start()
                return inner

            lax.fori_loop(1, members, give, 0)
            pltpu.make_async_copy(
                tri_part(group, chunk, spot, col), slot, recv_tri.at[chunk]
            ).start()
            return carry

        lax.fori_loop(0, chunks, give_chunk, 0)

    def finish(chunk, carry):
        first = pl.multiple_of(chunk * CHUNK, CHUNK)
        arrived = back.at[:, chunk_rows(chunk), :]
        pltpu.make_async_copy(arrived, arrived, recv_tri.at[chunk]).wait()
        sums = back[:, pl.ds(first, CHUNK), :].astype(jnp.float32)
        center = jnp.mean(sums, axis=0, keepdims=True)
        deviate = sums - center
        spread = jnp.mean(deviate * deviate, axis=0, keepdims=True)
        scaled = deviate * lax.rsqrt(spread + 1e-05)
        planes[:hidden, :CHUNK, :] = scaled

        def one_row(local, inner):
            at = first + local
            chans_first = wide[pl.ds(local, hidden, stride=PITCH), :]
            tri_normed = (chans_first * gain_col[...] + bias_col[...]).astype(jnp.bfloat16)
            projected = lax.dot_general(
                tri_normed, w_out_ref[...], (((0,), (0,)), ((), ())), preferred_element_type=jnp.float32
            )
            out_ref[at] = (gates[at] * projected).astype(jnp.bfloat16)
            return inner

        lax.fori_loop(0, CHUNK, one_row, 0, unroll=2)
        pltpu.make_async_copy(
            out_ref.at[chunk_rows(chunk)], out_hbm.at[chunk_rows(chunk)], store_sem
        ).start()
        return carry

    lax.fori_loop(0, chunks, finish, 0)
    pltpu.make_async_copy(out_ref, out_hbm, store_sem).wait()

    others = pl.ds(0, (members - 1) * share)
    pltpu.make_async_copy(edges.at[others], edges.at[others], send_left).wait()
    pltpu.make_async_copy(edges.at[others], edges.at[others], send_right.at[0]).wait()
    for turn in range(1, halves):
        every = pl.ds(0, hidden)
        pltpu.make_async_copy(edges.at[every], edges.at[every], send_right.at[turn]).wait()
    pltpu.make_async_copy(back.at[others], back.at[others], send_tri).wait()


def fused(rows_n, ka_n, halves, args):
    pair_repr, pair_mask, ln_gain, ln_bias, w_proj, w_gate, w_out_gate, out_gain, out_bias, w_out = args
    row_count, col_count, chans = pair_repr.shape
    hidden = w_out.shape[0]
    members = rows_n // halves * ka_n
    share = hidden // members
    groups = 2 if share % 2 == 0 else 1
    half = jnp.bfloat16
    return pl.pallas_call(
        functools.partial(kernel, rows_n, ka_n, halves, groups),
        out_shape=jax.ShapeDtypeStruct(pair_repr.shape, half),
        in_specs=[pl.BlockSpec(memory_space=pl.ANY)] + [pl.BlockSpec(memory_space=pltpu.VMEM)] * 9,
        out_specs=pl.BlockSpec(memory_space=pl.ANY),
        scratch_shapes=[
            pltpu.VMEM((row_count, col_count, chans), half),
            pltpu.VMEM((row_count, col_count, chans), half),
            pltpu.VMEM((2 * hidden, row_count, col_count), half),
            pltpu.VMEM((2 * hidden * PITCH, col_count), jnp.float32),
            pltpu.VMEM((row_count, col_count, chans), half),
            pltpu.VMEM((row_count, col_count, chans), jnp.float32),
            pltpu.VMEM((share, rows_n // halves * row_count, ka_n * col_count), half),
            pltpu.VMEM((share, rows_n * row_count, ka_n * col_count), half),
            pltpu.VMEM((share, rows_n // halves * row_count, ka_n * col_count), half),
            pltpu.VMEM((hidden, row_count, col_count), half),
            pltpu.VMEM((4 * hidden, chans), half),
            pltpu.VMEM((hidden, col_count), jnp.float32),
            pltpu.VMEM((hidden, col_count), jnp.float32),
            pltpu.SemaphoreType.DMA((row_count // CHUNK,)),
            pltpu.SemaphoreType.DMA,
            pltpu.SemaphoreType.DMA((groups,)),
            pltpu.SemaphoreType.DMA((groups,)),
            pltpu.SemaphoreType.DMA,
            pltpu.SemaphoreType.DMA((halves,)),
            pltpu.SemaphoreType.DMA((row_count // CHUNK,)),
            pltpu.SemaphoreType.DMA,
        ],
        compiler_params=pltpu.CompilerParams(
            collective_id=0, has_side_effects=True, vmem_limit_bytes=60 * 2**20
        ),
    )(
        pair_repr, pair_mask, ln_gain[None], ln_bias[None], w_proj, w_gate, w_out_gate,
        out_gain[None], out_bias[None], w_out,
    )


def plain(args):
    pair_repr, pair_mask, ln_gain, ln_bias, w_proj, w_gate, w_out_gate, out_gain, out_bias, w_out = args
    row_count, col_count, chans = pair_repr.shape
    hidden = w_out.shape[0]
    normed = layer_norm(pair_repr.astype(jnp.float32), ln_gain, ln_bias).astype(jnp.bfloat16)
    flat_rows = normed.reshape(row_count * col_count, chans)
    projected = jnp.dot(flat_rows, w_proj, preferred_element_type=jnp.float32)
    gate_logits = jnp.dot(flat_rows, w_gate, preferred_element_type=jnp.float32)
    mask_col = pair_mask.reshape(row_count * col_count, 1).astype(jnp.float32)
    edges = (jax.nn.sigmoid(gate_logits) * projected * mask_col).astype(jnp.bfloat16)
    edges = edges.reshape(row_count, col_count, 2 * hidden)
    partial_sums = jnp.einsum(
        "ikh,jkh->ijh",
        edges[:, :, :hidden],
        lax.all_gather(edges[:, :, hidden:], "rows", axis=0, tiled=True),
        preferred_element_type=jnp.float32,
    )
    triangle = lax.psum_scatter(
        partial_sums.astype(jnp.bfloat16), "ka", scatter_dimension=1, tiled=True
    ).astype(jnp.float32)
    tri_normed = layer_norm(triangle, out_gain, out_bias).astype(jnp.bfloat16)
    out_gate = jax.nn.sigmoid(jnp.dot(flat_rows, w_out_gate, preferred_element_type=jnp.float32))
    projected_out = jnp.dot(
        tri_normed.reshape(row_count * col_count, hidden), w_out, preferred_element_type=jnp.float32
    )
    return (out_gate * projected_out).astype(jnp.bfloat16).reshape(row_count, col_count, chans)


def body(rows_n, ka_n, *args):
    row_count, col_count, chans = args[0].shape
    hidden = args[-1].shape[0]
    halves = 2 if rows_n % 2 == 0 else 1
    members = rows_n // halves * ka_n
    aligned = row_count % CHUNK == 0 and col_count % 128 == 0 and chans % 128 == 0 and hidden % 128 == 0
    if aligned and hidden % members == 0 and col_count == hidden:
        return fused(rows_n, ka_n, halves, args)
    return plain(args)


def solution(mesh):
    placed = (P("rows", "ka", None), P("rows", "ka"), P(), P(), P(), P(), P(), P(), P(), P())
    return jax.shard_map(
        functools.partial(body, mesh.shape["rows"], mesh.shape["ka"]),
        mesh=mesh, in_specs=placed, out_specs=P("rows", "ka", None), check_vma=False,
    )
```
